32 devices in a mesh: stage: 4 (over z), data: 8 (over y, x, core).
Axes of the slice: x: 2, y: 2, z: 4, core: 2. Of those that a mesh axis runs over, the one named last changes fastest.
Arguments:
- tokens_in: bfloat16 [32, 64, 1280], P('data')
- targets: bfloat16 [32, 64, 1280], P('data')
- w_up: bfloat16 [2, 4, 1280, 5120], P(None, 'stage')
- w_down: bfloat16 [2, 4, 5120, 1280], P(None, 'stage')
Outputs:
- output 1: float32 [], replicated
- output 2: float32 [2, 4, 1280, 5120], P(None, 'stage', 'data')
- output 3: float32 [2, 4, 5120, 1280], P(None, 'stage', 'data')
All inputs are finite; a program needn't handle non-finite values.
Results may differ from the reference program's by a relative error of at most 0.00283349.
Values are sent between devices in bfloat16 or wider.
A program may use at most 1 GiB of HBM per device.

```python
import jax
import jax.numpy as jnp
from jax import lax

D_MODEL = 1280
FF = 5120
TOKENS = 64
BATCH_MB = 32
HALF_LAYERS = 4
N_LAYERS = 2 * HALF_LAYERS
N_TOKENS = BATCH_MB * TOKENS


def setup_inputs(seed: int = 0) -> dict:
    key_list = jax.random.split(jax.random.key(seed), 8)
    noise_in = jax.random.normal(key_list[0], (BATCH_MB, TOKENS, D_MODEL), jnp.float32)
    shift_in = 2.0 * jax.random.normal(key_list[1], (BATCH_MB, 1, D_MODEL), jnp.float32)
    noise_out = jax.random.normal(key_list[2], (BATCH_MB, TOKENS, D_MODEL), jnp.float32)
    shift_out = 2.0 * jax.random.normal(key_list[3], (BATCH_MB, 1, D_MODEL), jnp.float32)
    in_gain = jnp.exp(jax.random.uniform(key_list[6], (), jnp.float32, -0.8, 0.8))
    out_gain = jnp.exp(jax.random.uniform(key_list[7], (), jnp.float32, -1.0, 1.0))
    up_scale = D_MODEL ** -0.5
    down_scale = (2.0 / (N_LAYERS * FF)) ** 0.5
    w_up = up_scale * jax.random.normal(key_list[4], (2, HALF_LAYERS, D_MODEL, FF), jnp.float32)
    w_down = down_scale * jax.random.normal(key_list[5], (2, HALF_LAYERS, FF, D_MODEL), jnp.float32)
    return {
        "tokens_in": ((noise_in + shift_in) * in_gain).astype(jnp.bfloat16),
        "targets": ((noise_out + shift_out) * out_gain).astype(jnp.bfloat16),
        "w_up": w_up.astype(jnp.bfloat16),
        "w_down": w_down.astype(jnp.bfloat16),
    }


def gelu_fn(pre_act):
    return jax.nn.gelu(pre_act, approximate=True)


def layer_fwd(h_in, w_one, w_two):
    pre_act = jnp.dot(h_in, w_one, preferred_element_type=jnp.float32)
    act_bf = gelu_fn(pre_act).astype(jnp.bfloat16)
    out_val = h_in.astype(jnp.float32) + jnp.dot(act_bf, w_two, preferred_element_type=jnp.float32)
    return out_val.astype(jnp.bfloat16)


def layer_bwd(h_in, grad_out, w_one, w_two):
    pre_act = jnp.dot(h_in, w_one, preferred_element_type=jnp.float32)
    act_val, gelu_vjp = jax.vjp(gelu_fn, pre_act)
    act_bf = act_val.astype(jnp.bfloat16)
    g_down = jnp.dot(act_bf.T, grad_out, preferred_element_type=jnp.float32)
    d_act = jnp.dot(grad_out, w_two.T, preferred_element_type=jnp.float32).astype(jnp.bfloat16)
    d_pre = gelu_vjp(d_act.astype(jnp.float32))[0].astype(jnp.bfloat16)
    g_up = jnp.dot(h_in.T, d_pre, preferred_element_type=jnp.float32)
    back_val = jnp.dot(d_pre, w_one.T, preferred_element_type=jnp.float32)
    d_in = (grad_out.astype(jnp.float32) + back_val).astype(jnp.bfloat16)
    return d_in, g_up, g_down


def reference(tokens_in, targets, w_up, w_down):
    up_flat = w_up.reshape(N_LAYERS, D_MODEL, FF)
    down_flat = w_down.reshape(N_LAYERS, FF, D_MODEL)

    def fwd_body(h_cur, layer_w):
        return layer_fwd(h_cur, layer_w[0], layer_w[1]), h_cur

    def bwd_body(g_cur, layer_items):
        d_in, g_up, g_down = layer_bwd(layer_items[0], g_cur, layer_items[1], layer_items[2])
        return d_in, (g_up, g_down)

    def micro_step(scan_state, mb_pair):
        loss_acc, acc_up, acc_down = scan_state
        h_last, saved_in = lax.scan(fwd_body, mb_pair[0], (up_flat, down_flat))
        out_err = h_last.astype(jnp.float32) - mb_pair[1].astype(jnp.float32)
        loss_acc = loss_acc + jnp.sum(out_err * out_err) / (2.0 * N_TOKENS)
        grad_top = (out_err / N_TOKENS).astype(jnp.bfloat16)
        _, (g_ups, g_downs) = lax.scan(bwd_body, grad_top, (saved_in, up_flat, down_flat), reverse=True)
        return (loss_acc, acc_up + g_ups, acc_down + g_downs), None

    init_state = (
        jnp.zeros((), jnp.float32),
        jnp.zeros((N_LAYERS, D_MODEL, FF), jnp.float32),
        jnp.zeros((N_LAYERS, FF, D_MODEL), jnp.float32),
    )
    (loss, acc_up, acc_down), _ = lax.scan(micro_step, init_state, (tokens_in, targets))
    return loss, acc_up.reshape(2, HALF_LAYERS, D_MODEL, FF), acc_down.reshape(2, HALF_LAYERS, FF, D_MODEL)
```

```python
import jax
import jax.numpy as jnp
from jax import lax
from jax.sharding import PartitionSpec as P


def gelu_fn(pre_act):
    return jax.nn.gelu(pre_act, approximate=True)


def matmul(lhs, rhs, dims):
    return lax.dot_general(lhs, rhs, (dims, ((), ())), preferred_element_type=jnp.float32)


def layer_fwd(h_in, w_one, w_two):
    act = gelu_fn(matmul(h_in, w_one, ((1,), (0,)))).astype(jnp.bfloat16)
    out_val = h_in.astype(jnp.float32) + matmul(act, w_two, ((1,), (0,)))
    return out_val.astype(jnp.bfloat16)


def act_bwd(h_in, grad_out, w_one, w_two):
    pre_act = matmul(h_in, w_one, ((1,), (0,)))
    act_val, gelu_vjp = jax.vjp(gelu_fn, pre_act)
    d_act = matmul(grad_out, w_two, ((1,), (1,))).astype(jnp.bfloat16)
    d_pre = gelu_vjp(d_act.astype(jnp.float32))[0].astype(jnp.bfloat16)
    return act_val.astype(jnp.bfloat16), d_pre


def layer_dgrad(h_in, grad_out, w_one, w_two):
    _, d_pre = act_bwd(h_in, grad_out, w_one, w_two)
    back_val = matmul(d_pre, w_one, ((1,), (1,)))
    return (grad_out.astype(jnp.float32) + back_val).astype(jnp.bfloat16)


def put_slot(buf, val, idx):
    return lax.dynamic_update_slice(buf, val[None], (idx, 0, 0))


def solution(mesh):
    n_stage = mesh.shape["stage"]
    n_data = mesh.shape["data"]

    def device_fn(tokens_loc, targets_loc, up_loc, down_loc):
        n_micro, seq_len, d_model = tokens_loc.shape
        d_ff = up_loc.shape[3]
        n_tok = n_data * n_micro * seq_len
        n_slots = 2 * n_micro
        stage_idx = lax.axis_index("stage")
        data_idx = lax.axis_index("data")
        is_first = stage_idx == 0
        is_last = stage_idx == n_stage - 1
        fwd_perm = [(src, (src + 1) % n_stage) for src in range(n_stage)]
        bwd_perm = [(src, (src - 1) % n_stage) for src in range(n_stage)]
        up_loc = up_loc[:, 0]
        down_loc = down_loc[:, 0]

        def pick(arr, idx):
            return lax.dynamic_index_in_dim(arr, idx, 0, keepdims=False)

        def fwd_slot(tick_idx, state):
            h_in, stash, tops, loss = state
            slot = tick_idx - stage_idx
            valid = (slot >= 0) & (slot < n_slots)
            slot = jnp.clip(slot, 0, n_slots - 1)
            virt = slot // n_micro
            micro = slot % n_micro
            h_cur = jnp.where(is_first & (virt == 0), pick(tokens_loc, micro), h_in)
            stash = put_slot(stash, h_cur, jnp.where(valid, slot, n_slots))
            h_out = layer_fwd(h_cur, pick(up_loc, virt), pick(down_loc, virt))
            err = h_out.astype(jnp.float32) - pick(targets_loc, micro).astype(jnp.float32)
            is_top = is_last & valid & (virt == 1)
            loss = loss + jnp.where(is_top, jnp.sum(err * err) / (2.0 * n_tok), 0.0)
            tops = put_slot(tops, (err / n_tok).astype(jnp.bfloat16), jnp.where(is_top, micro, n_micro))
            return lax.ppermute(h_out, "stage", fwd_perm), stash, tops, loss

        def bwd_slot(tick_idx, state):
            g_in, gstash = state
            slot = tick_idx - (n_stage - 1 - stage_idx)
            valid = (slot >= 0) & (slot < n_slots)
            slot = jnp.clip(slot, 0, n_slots - 1)
            virt = 1 - slot // n_micro
            micro = slot % n_micro
            g_cur = jnp.where(is_last & (virt == 1), pick(tops, micro), g_in)
            pos = virt * n_micro + micro
            gstash = put_slot(gstash, g_cur, jnp.where(valid, pos, n_slots))
            g_out = layer_dgrad(pick(stash, pos), g_cur, pick(up_loc, virt), pick(down_loc, virt))
            return lax.ppermute(g_out, "stage", bwd_perm), gstash

        n_ticks = n_slots + n_stage - 1
        zero_act = jnp.zeros((seq_len, d_model), jnp.bfloat16)
        stash0 = jnp.zeros((n_slots + 1, seq_len, d_model), jnp.bfloat16)
        tops0 = jnp.zeros((n_micro + 1, seq_len, d_model), jnp.bfloat16)
        _, stash, tops, loss = lax.fori_loop(0, n_ticks, fwd_slot, (zero_act, stash0, tops0, jnp.zeros((), jnp.float32)))
        _, gstash = lax.fori_loop(0, n_ticks, bwd_slot, (zero_act, stash0))

        f_loc = d_ff // n_data
        ups, downs = [], []
        for virt in range(2):
            h_all = lax.all_gather(stash[virt * n_micro:(virt + 1) * n_micro].reshape(-1, d_model), "data", tiled=True)
            g_all = lax.all_gather(gstash[virt * n_micro:(virt + 1) * n_micro].reshape(-1, d_model), "data", tiled=True)
            w_one = lax.dynamic_slice(up_loc[virt], (0, data_idx * f_loc), (d_model, f_loc))
            w_two = lax.dynamic_slice(down_loc[virt], (data_idx * f_loc, 0), (f_loc, d_model))
            act, d_pre = act_bwd(h_all, g_all, w_one, w_two)
            downs.append(matmul(act, g_all, ((0,), (0,))))
            g_up = matmul(h_all, d_pre, ((0,), (0,)))
            ups.append(lax.all_to_all(g_up, "data", 0, 1, tiled=True))
        loss = lax.psum(loss, ("stage", "data"))
        return loss, jnp.stack(ups)[:, None], jnp.stack(downs)[:, None]

    return jax.shard_map(
        device_fn,
        mesh=mesh,
        in_specs=(P("data"), P("data"), P(None, "stage"), P(None, "stage")),
        out_specs=(P(), P(None, "stage", "data"), P(None, "stage", "data")),
        check_vma=False,
    )
```

```python
import functools

import jax
import jax.numpy as jnp
import numpy as np
from jax import lax
from jax.experimental import pallas as pl
from jax.experimental.pallas import tpu as pltpu
from jax.sharding import PartitionSpec as P

BF = jnp.bfloat16
F32 = jnp.float32
MESH = pl.DeviceIdType.MESH
VMEM_BYTES = 67043328


def gelu_fn(pre_act):
    return jax.nn.gelu(pre_act, approximate=True)


def gelu_and_slope(pre_act):
    c_one, c_two = np.float32(np.sqrt(2.0 / np.pi)), np.float32(0.044715)
    square = pre_act * pre_act
    tanh = jnp.tanh(c_one * (pre_act + c_two * (square * pre_act)))
    cdf = 0.5 * (1.0 + tanh)
    inner = c_one + (c_one * 3 * c_two) * square
    return pre_act * cdf, cdf + (0.5 * pre_act) * ((1.0 - tanh * tanh) * inner)


def matmul(lhs, rhs, dims):
    return lax.dot_general(lhs, rhs, (dims, ((), ())), preferred_element_type=F32)


class Place:
    def __init__(self, n_stage):
        self.stage = lax.axis_index("stage")
        self.data = lax.axis_index("data")
        core = lax.rem(self.data, 2)
        x = lax.rem(lax.div(self.data, 2), 2)
        y = lax.div(self.data, 4)
        self.partner = self.data + 1 - 2 * core
        dx, dy = 2 - 4 * x, 4 - 8 * y
        self.moves = (dx, dy, dx + dy)
        self.next = lax.rem(self.stage + 1, n_stage)
        self.prev = lax.rem(self.stage + n_stage - 1, n_stage)

    def at(self, stage, data):
        return {"stage": stage, "data": data}

    def peers(self):
        yield self.at(self.next, self.data)
        yield self.at(self.prev, self.data)
        yield self.at(self.stage, self.partner)
        for move in self.moves:
            yield self.at(self.stage, self.data + move)

    def barrier(self):
        sem = pltpu.get_barrier_semaphore()
        for peer in self.peers():
            pl.semaphore_signal(sem, inc=1, device_id=peer, device_id_type=MESH)
        pl.semaphore_wait(sem, 6)


def remote(src, dst, send_sem, recv_sem, device):
    return pltpu.make_async_remote_copy(
        src_ref=src, dst_ref=dst, send_sem=send_sem, recv_sem=recv_sem, device_id=device, device_id_type=MESH
    )


class Spread:
    def __init__(self, place, src, dst, n_micro, sems):
        self.place, self.src, self.dst, self.n_micro = place, src, dst, n_micro
        self.own_sem, self.send_sem, self.recv_sem, self.fsend_sem, self.frecv_sem = sems

    def spot(self, slot, data):
        return self.dst.at[lax.div(slot, self.n_micro), data, lax.rem(slot, self.n_micro)]

    def own(self, slot):
        return pltpu.make_async_copy(self.src.at[slot], self.spot(slot, self.place.data), self.own_sem.at[slot])

    def direct(self, slot, k):
        place = self.place
        peer = place.partner if k == 0 else place.data + place.moves[k - 1]
        return remote(
            self.src.at[slot],
            self.spot(slot, place.data),
            self.send_sem.at[slot, k],
            self.recv_sem.at[slot, k],
            place.at(place.stage, peer),
        )

    def relay(self, slot, k):
        place = self.place
        spot = self.spot(slot, place.data + place.moves[k])
        return remote(
            spot, spot, self.fsend_sem.at[slot, k], self.frecv_sem.at[slot, k], place.at(place.stage, place.partner)
        )

    def send(self, slot):
        self.own(slot).start()
        for k in range(4):
            self.direct(slot, k).start()

    def forward(self, slot):
        for k in range(3):
            self.direct(slot, k + 1).wait_recv()
            self.relay(slot, k).start()

    def finish(self, n_slots):
        def body(slot, carry):
            self.own(slot).wait()
            self.direct(slot, 0).wait_recv()
            for k in range(4):
                self.direct(slot, k).wait_send()
            for k in range(3):
                self.relay(slot, k).wait()
            return carry

        lax.fori_loop(0, n_slots, body, 0)


def spread_sems(n_slots):
    dma = pltpu.SemaphoreType.DMA
    return [dma((n_slots,)), dma((n_slots, 4)), dma((n_slots, 4)), dma((n_slots, 3)), dma((n_slots, 3))]


def fwd_kernel(
    n_stage, n_tok, tok_ref, tgt_ref, up_ref, down_ref, hg_ref, slope_ref, top_ref, loss_ref,
    w_up, w_down, h_in, h_out, act, slope, tgt, top, loss,
    up_sem, down_sem, tok_sem, tgt_sem, slope_sem, top_sem, zsend_sem, zrecv_sem, *spread,
):
    n_micro = tok_ref.shape[0]
    n_slots = 2 * n_micro
    d_model, d_ff = w_up.shape[1:]
    up_cols = d_ff // up_sem.shape[1]
    down_cols = d_model // down_sem.shape[1]
    place = Place(n_stage)
    is_first = place.stage == 0
    is_last = place.stage == n_stage - 1

    def load_tok(i):
        return pltpu.make_async_copy(tok_ref.at[i], h_in.at[i], tok_sem.at[i])

    def load_up(v, c):
        cols = pl.ds(c * up_cols, up_cols)
        return pltpu.make_async_copy(up_ref.at[v, 0, :, cols], w_up.at[v, :, cols], up_sem.at[v, c])

    def load_down(v, c):
        cols = pl.ds(c * down_cols, down_cols)
        return pltpu.make_async_copy(down_ref.at[v, 0, :, cols], w_down.at[v, :, cols], down_sem.at[v, c])

    @pl.when(is_first)
    def _():
        for i in range(n_micro):
            load_tok(i).start()

    for v in range(2):
        for c in range(up_sem.shape[1]):
            load_up(v, c).start()
        for c in range(down_sem.shape[1]):
            load_down(v, c).start()
    load_tgt = pltpu.make_async_copy(tgt_ref, tgt, tgt_sem)
    load_tgt.start()
    loss[...] = jnp.zeros_like(loss)
    place.barrier()
    gather = Spread(place, h_in, hg_ref, n_micro, spread)

    def put_slope(slot):
        v, i, b = lax.div(slot, n_micro), lax.rem(slot, n_micro), lax.rem(slot, 2)
        return pltpu.make_async_copy(slope.at[b], slope_ref.at[v, i], slope_sem.at[b])

    def hand_on(slot):
        to = slot + n_micro * lax.div(place.stage, n_stage - 1)
        return remote(
            h_out.at[slot], h_in.at[to], zsend_sem.at[slot], zrecv_sem.at[to], place.at(place.next, place.data)
        )

    def arrive(slot):
        return remote(
            h_out.at[slot], h_in.at[slot], zsend_sem.at[slot], zrecv_sem.at[slot], place.at(place.next, place.data)
        )

    def body(slot, carry):
        v, i, b = lax.div(slot, n_micro), lax.rem(slot, n_micro), lax.rem(slot, 2)
        from_data = jnp.logical_and(is_first, v == 0)
        is_top = jnp.logical_and(is_last, v == 1)

        @pl.when(from_data)
        def _():
            load_tok(i).wait()

        @pl.when(jnp.logical_not(from_data))
        def _():
            arrive(slot).wait_recv()

        gather.send(slot)

        @pl.when(i == 0)
        def _():
            for c in range(up_sem.shape[1]):
                load_up(v, c).wait()

        @pl.when(slot >= 2)
        def _():
            put_slope(slot - 2).wait()

        for c in range(up_sem.shape[1]):
            cols = slice(c * up_cols, (c + 1) * up_cols)
            pre_act = matmul(h_in[slot], w_up[v, :, cols], ((1,), (0,)))
            act_val, slope_val = gelu_and_slope(pre_act)
            act[:, cols] = act_val.astype(BF)
            slope[b, :, cols] = slope_val
        put_slope(slot).start()

        @pl.when(i == 0)
        def _():
            for c in range(down_sem.shape[1]):
                load_down(v, c).wait()

        for c in range(down_sem.shape[1]):
            cols = slice(c * down_cols, (c + 1) * down_cols)
            out_val = matmul(act[...], w_down[v, :, cols], ((1,), (0,)))
            h_out[slot, :, cols] = (h_in[slot, :, cols].astype(F32) + out_val).astype(BF)

        @pl.when(jnp.logical_not(is_top))
        def _():
            hand_on(slot).start()

        @pl.when(is_top)
        def _():
            @pl.when(i == 0)
            def _():
                load_tgt.wait()

            for c in range(d_model // 128):
                cols = slice(c * 128, (c + 1) * 128)
                err = h_out[slot, :, cols].astype(F32) - tgt[i, :, cols].astype(F32)
                loss[...] += err * err
                top[i, :, cols] = (err / n_tok).astype(BF)

        @pl.when(slot >= 2)
        def _():
            gather.forward(slot - 2)

        return carry

    lax.fori_loop(0, n_slots, body, 0)
    loss_ref[...] = loss[...]
    put_top = pltpu.make_async_copy(top, top_ref, top_sem)

    @pl.when(is_last)
    def _():
        put_top.start()

    @pl.when(jnp.logical_not(is_last))
    def _():
        load_tgt.wait()

    gather.forward(n_slots - 2)
    gather.forward(n_slots - 1)
    gather.finish(n_slots)
    put_slope(n_slots - 2).wait()
    put_slope(n_slots - 1).wait()
    n_sent = n_slots - n_micro * lax.div(place.stage, n_stage - 1)

    def drain(slot, carry):
        hand_on(slot).wait_send()
        return carry

    lax.fori_loop(0, n_sent, drain, 0)

    @pl.when(is_last)
    def _():
        put_top.wait()


def forward(n_stage, n_data, tokens, targets, up, down):
    n_micro, seq_len, d_model = tokens.shape
    d_ff = up.shape[3]
    n_slots = 2 * n_micro
    dma = pltpu.SemaphoreType.DMA
    hbm = pl.BlockSpec(memory_space=pl.ANY)
    act_shape = (seq_len, d_model)
    return pl.pallas_call(
        functools.partial(fwd_kernel, n_stage, n_data * n_micro * seq_len),
        out_shape=(
            jax.ShapeDtypeStruct((2, n_data, n_micro, *act_shape), BF),
            jax.ShapeDtypeStruct((2, n_micro, seq_len, d_ff), F32),
            jax.ShapeDtypeStruct((n_micro, *act_shape), BF),
            jax.ShapeDtypeStruct((seq_len, 128), F32),
        ),
        in_specs=[hbm] * 4,
        out_specs=(hbm, hbm, hbm, pl.BlockSpec(memory_space=pltpu.VMEM)),
        scratch_shapes=[
            pltpu.VMEM((2, d_model, d_ff), BF),
            pltpu.VMEM((2, d_ff, d_model), BF),
            pltpu.VMEM((n_slots, *act_shape), BF),
            pltpu.VMEM((n_slots, *act_shape), BF),
            pltpu.VMEM((seq_len, d_ff), BF),
            pltpu.VMEM((2, seq_len, d_ff), F32),
            pltpu.VMEM((n_micro, *act_shape), BF),
            pltpu.VMEM((n_micro, *act_shape), BF),
            pltpu.VMEM((seq_len, 128), F32),
            dma((2, 4)), dma((2, 2)), dma((n_micro,)), dma, dma((2,)), dma, dma((n_slots,)), dma((n_slots,)),
            *spread_sems(n_slots),
        ],
        compiler_params=pltpu.CompilerParams(collective_id=0, has_side_effects=True, vmem_limit_bytes=VMEM_BYTES),
        name="fwd_pipe",
    )(tokens, targets, up, down)


def act_bwd(h_in, grad_out, w_one, w_two):
    act_val, gelu_vjp = jax.vjp(gelu_fn, matmul(h_in, w_one, ((1,), (0,))))
    d_act = matmul(grad_out, w_two, ((1,), (1,))).astype(BF)
    d_pre = gelu_vjp(d_act.astype(F32))[0].astype(BF)
    return act_val.astype(BF), d_pre


def layer_dgrad(slope, grad_out, w_one, w_two):
    d_act = matmul(grad_out, w_two, ((1,), (1,))).astype(BF)
    d_pre = (slope * d_act.astype(F32)).astype(BF)
    return (grad_out.astype(F32) + matmul(d_pre, w_one, ((1,), (1,)))).astype(BF)


def put_slot(buf, val, idx):
    return lax.dynamic_update_slice(buf, val[None], (idx, 0, 0))


def solution(mesh):
    n_stage = mesh.shape["stage"]
    n_data = mesh.shape["data"]

    def device_fn(tokens_loc, targets_loc, up_loc, down_loc):
        n_micro, seq_len, d_model = tokens_loc.shape
        d_ff = up_loc.shape[3]
        n_tok = n_data * n_micro * seq_len
        n_slots = 2 * n_micro
        stage_idx = lax.axis_index("stage")
        data_idx = lax.axis_index("data")
        is_last = stage_idx == n_stage - 1
        bwd_perm = [(src, (src - 1) % n_stage) for src in range(n_stage)]

        h_all, slope, tops, loss = forward(n_stage, n_data, tokens_loc, targets_loc, up_loc, down_loc)
        up_loc = up_loc[:, 0]
        down_loc = down_loc[:, 0]
        slope = slope.reshape(n_slots, seq_len, d_ff)

        def pick(arr, idx):
            return lax.dynamic_index_in_dim(arr, idx, 0, keepdims=False)

        def bwd_slot(tick_idx, state):
            g_in, gstash = state
            slot = tick_idx - (n_stage - 1 - stage_idx)
            valid = (slot >= 0) & (slot < n_slots)
            slot = jnp.clip(slot, 0, n_slots - 1)
            virt = 1 - slot // n_micro
            micro = slot % n_micro
            g_cur = jnp.where(is_last & (virt == 1), pick(tops, micro), g_in)
            pos = virt * n_micro + micro
            gstash = put_slot(gstash, g_cur, jnp.where(valid, pos, n_slots))
            g_out = layer_dgrad(pick(slope, pos), g_cur, pick(up_loc, virt), pick(down_loc, virt))
            return lax.ppermute(g_out, "stage", bwd_perm), gstash

        n_ticks = n_slots + n_stage - 1
        zero_act = jnp.zeros((seq_len, d_model), BF)
        stash0 = jnp.zeros((n_slots + 1, seq_len, d_model), BF)
        _, gstash = lax.fori_loop(0, n_ticks, bwd_slot, (zero_act, stash0))

        f_loc = d_ff // n_data
        ups, downs = [], []
        for virt in range(2):
            h_one = h_all[virt].reshape(-1, d_model)
            g_one = lax.all_gather(gstash[virt * n_micro : (virt + 1) * n_micro].reshape(-1, d_model), "data", tiled=True)
            w_one = lax.dynamic_slice(up_loc[virt], (0, data_idx * f_loc), (d_model, f_loc))
            w_two = lax.dynamic_slice(down_loc[virt], (data_idx * f_loc, 0), (f_loc, d_model))
            act, d_pre = act_bwd(h_one, g_one, w_one, w_two)
            downs.append(matmul(act, g_one, ((0,), (0,))))
            g_up = matmul(h_one, d_pre, ((0,), (0,)))
            ups.append(lax.all_to_all(g_up, "data", 0, 1, tiled=True))
        loss = lax.psum(jnp.sum(loss) / (2.0 * n_tok), ("stage", "data"))
        return loss, jnp.stack(ups)[:, None], jnp.stack(downs)[:, None]

    return jax.shard_map(
        device_fn,
        mesh=mesh,
        in_specs=(P("data"), P("data"), P(None, "stage"), P(None, "stage")),
        out_specs=(P(), P(None, "stage", "data"), P(None, "stage", "data")),
        check_vma=False,
    )
```

```python
import functools

import jax
import jax.numpy as jnp
import numpy as np
from jax import lax
from jax.experimental import pallas as pl
from jax.experimental.pallas import tpu as pltpu
from jax.sharding import PartitionSpec as P

BF = jnp.bfloat16
F32 = jnp.float32
MESH = pl.DeviceIdType.MESH
VMEM_BYTES = 67043328


def gelu_fn(pre_act):
    return jax.nn.gelu(pre_act, approximate=True)


def gelu_and_slope(pre_act):
    c_one, c_two = np.float32(np.sqrt(2.0 / np.pi)), np.float32(0.044715)
    square = pre_act * pre_act
    tanh = jnp.tanh(c_one * (pre_act + c_two * (square * pre_act)))
    cdf = 0.5 * (1.0 + tanh)
    inner = c_one + (c_one * 3 * c_two) * square
    return pre_act * cdf, cdf + (0.5 * pre_act) * ((1.0 - tanh * tanh) * inner)


def matmul(lhs, rhs, dims):
    return lax.dot_general(lhs, rhs, (dims, ((), ())), preferred_element_type=F32)


class Place:
    def __init__(self, n_stage):
        self.stage = lax.axis_index("stage")
        self.data = lax.axis_index("data")
        core = lax.rem(self.data, 2)
        x = lax.rem(lax.div(self.data, 2), 2)
        y = lax.div(self.data, 4)
        self.partner = self.data + 1 - 2 * core
        dx, dy = 2 - 4 * x, 4 - 8 * y
        self.moves = (dx, dy, dx + dy)
        self.next = lax.rem(self.stage + 1, n_stage)
        self.prev = lax.rem(self.stage + n_stage - 1, n_stage)

    def at(self, stage, data):
        return {"stage": stage, "data": data}

    def peers(self):
        yield self.at(self.next, self.data)
        yield self.at(self.prev, self.data)
        yield self.at(self.stage, self.partner)
        for move in self.moves:
            yield self.at(self.stage, self.data + move)

    def barrier(self):
        sem = pltpu.get_barrier_semaphore()
        for peer in self.peers():
            pl.semaphore_signal(sem, inc=1, device_id=peer, device_id_type=MESH)
        pl.semaphore_wait(sem, 6)


def remote(src, dst, send_sem, recv_sem, device):
    return pltpu.make_async_remote_copy(
        src_ref=src, dst_ref=dst, send_sem=send_sem, recv_sem=recv_sem, device_id=device, device_id_type=MESH
    )


class Spread:
    def __init__(self, place, src, dst, n_micro, sems):
        self.place, self.src, self.dst, self.n_micro = place, src, dst, n_micro
        self.own_sem, self.send_sem, self.recv_sem, self.fsend_sem, self.frecv_sem = sems

    def spot(self, slot, data):
        return self.dst.at[lax.div(slot, self.n_micro), data, lax.rem(slot, self.n_micro)]

    def own(self, slot):
        return pltpu.make_async_copy(self.src.at[slot], self.spot(slot, self.place.data), self.own_sem.at[slot])

    def direct(self, slot, k):
        place = self.place
        peer = place.partner if k == 0 else place.data + place.moves[k - 1]
        return remote(
            self.src.at[slot],
            self.spot(slot, place.data),
            self.send_sem.at[slot, k],
            self.recv_sem.at[slot, k],
            place.at(place.stage, peer),
        )

    def relay(self, slot, k):
        place = self.place
        spot = self.spot(slot, place.data + place.moves[k])
        return remote(
            spot, spot, self.fsend_sem.at[slot, k], self.frecv_sem.at[slot, k], place.at(place.stage, place.partner)
        )

    def send(self, slot):
        self.own(slot).start()
        for k in range(4):
            self.direct(slot, k).start()

    def forward(self, slot):
        for k in range(3):
            self.direct(slot, k + 1).wait_recv()
            self.relay(slot, k).start()

    def finish(self, n_slots):
        def body(slot, carry):
            self.own(slot).wait()
            self.direct(slot, 0).wait_recv()
            for k in range(4):
                self.direct(slot, k).wait_send()
            for k in range(3):
                self.relay(slot, k).wait()
            return carry

        lax.fori_loop(0, n_slots, body, 0)


def spread_sems(n_slots):
    dma = pltpu.SemaphoreType.DMA
    return [dma((n_slots,)), dma((n_slots, 4)), dma((n_slots, 4)), dma((n_slots, 3)), dma((n_slots, 3))]


def fwd_kernel(
    n_stage, n_tok, tok_ref, tgt_ref, up_ref, down_ref, hg_ref, slope_ref, top_ref, loss_ref,
    w_up, w_down, h_in, h_out, act, slope, tgt, top, loss,
    up_sem, down_sem, tok_sem, tgt_sem, slope_sem, top_sem, zsend_sem, zrecv_sem, *spread,
):
    n_micro = tok_ref.shape[0]
    n_slots = 2 * n_micro
    d_model, d_ff = w_up.shape[1:]
    up_cols = d_ff // up_sem.shape[1]
    down_cols = d_model // down_sem.shape[1]
    place = Place(n_stage)
    is_first = place.stage == 0
    is_last = place.stage == n_stage - 1

    def load_tok(i):
        return pltpu.make_async_copy(tok_ref.at[i], h_in.at[i], tok_sem.at[i])

    def load_up(v, c):
        cols = pl.ds(c * up_cols, up_cols)
        return pltpu.make_async_copy(up_ref.at[v, 0, :, cols], w_up.at[v, :, cols], up_sem.at[v, c])

    def load_down(v, c):
        cols = pl.ds(c * down_cols, down_cols)
        return pltpu.make_async_copy(down_ref.at[v, 0, :, cols], w_down.at[v, :, cols], down_sem.at[v, c])

    @pl.when(is_first)
    def _():
        for i in range(n_micro):
            load_tok(i).start()

    for v in range(2):
        for c in range(up_sem.shape[1]):
            load_up(v, c).start()
        for c in range(down_sem.shape[1]):
            load_down(v, c).start()
    load_tgt = pltpu.make_async_copy(tgt_ref, tgt, tgt_sem)
    load_tgt.start()
    loss[...] = jnp.zeros_like(loss)
    place.barrier()
    gather = Spread(place, h_in, hg_ref, n_micro, spread)

    def put_slope(slot):
        v, i, b = lax.div(slot, n_micro), lax.rem(slot, n_micro), lax.rem(slot, 2)
        return pltpu.make_async_copy(slope.at[b], slope_ref.at[v, i], slope_sem.at[b])

    def hand_on(slot):
        to = slot + n_micro * lax.div(place.stage, n_stage - 1)
        return remote(
            h_out.at[slot], h_in.at[to], zsend_sem.at[slot], zrecv_sem.at[to], place.at(place.next, place.data)
        )

    def arrive(slot):
        return remote(
            h_out.at[slot], h_in.at[slot], zsend_sem.at[slot], zrecv_sem.at[slot], place.at(place.next, place.data)
        )

    def body(slot, carry):
        v, i, b = lax.div(slot, n_micro), lax.rem(slot, n_micro), lax.rem(slot, 2)
        from_data = jnp.logical_and(is_first, v == 0)
        is_top = jnp.logical_and(is_last, v == 1)

        @pl.when(from_data)
        def _():
            load_tok(i).wait()

        @pl.when(jnp.logical_not(from_data))
        def _():
            arrive(slot).wait_recv()

        gather.send(slot)

        @pl.when(i == 0)
        def _():
            for c in range(up_sem.shape[1]):
                load_up(v, c).wait()

        @pl.when(slot >= 2)
        def _():
            put_slope(slot - 2).wait()

        for c in range(up_sem.shape[1]):
            cols = slice(c * up_cols, (c + 1) * up_cols)
            pre_act = matmul(h_in[slot], w_up[v, :, cols], ((1,), (0,)))
            act_val, slope_val = gelu_and_slope(pre_act)
            act[:, cols] = act_val.astype(BF)
            slope[b, :, cols] = slope_val
        put_slope(slot).start()

        @pl.when(i == 0)
        def _():
            for c in range(down_sem.shape[1]):
                load_down(v, c).wait()

        for c in range(down_sem.shape[1]):
            cols = slice(c * down_cols, (c + 1) * down_cols)
            out_val = matmul(act[...], w_down[v, :, cols], ((1,), (0,)))
            h_out[slot, :, cols] = (h_in[slot, :, cols].astype(F32) + out_val).astype(BF)

        @pl.when(jnp.logical_not(is_top))
        def _():
            hand_on(slot).start()

        @pl.when(is_top)
        def _():
            @pl.when(i == 0)
            def _():
                load_tgt.wait()

            for c in range(d_model // 128):
                cols = slice(c * 128, (c + 1) * 128)
                err = h_out[slot, :, cols].astype(F32) - tgt[i, :, cols].astype(F32)
                loss[...] += err * err
                top[i, :, cols] = (err / n_tok).astype(BF)

        @pl.when(slot >= 2)
        def _():
            gather.forward(slot - 2)

        return carry

    lax.fori_loop(0, n_slots, body, 0)
    loss_ref[...] = loss[...]
    put_top = pltpu.make_async_copy(top, top_ref, top_sem)

    @pl.when(is_last)
    def _():
        put_top.start()

    @pl.when(jnp.logical_not(is_last))
    def _():
        load_tgt.wait()

    gather.forward(n_slots - 2)
    gather.forward(n_slots - 1)
    gather.finish(n_slots)
    put_slope(n_slots - 2).wait()
    put_slope(n_slots - 1).wait()
    n_sent = n_slots - n_micro * lax.div(place.stage, n_stage - 1)

    def drain(slot, carry):
        hand_on(slot).wait_send()
        return carry

    lax.fori_loop(0, n_sent, drain, 0)

    @pl.when(is_last)
    def _():
        put_top.wait()


def forward(n_stage, n_data, tokens, targets, up, down):
    n_micro, seq_len, d_model = tokens.shape
    d_ff = up.shape[3]
    n_slots = 2 * n_micro
    dma = pltpu.SemaphoreType.DMA
    hbm = pl.BlockSpec(memory_space=pl.ANY)
    act_shape = (seq_len, d_model)
    return pl.pallas_call(
        functools.partial(fwd_kernel, n_stage, n_data * n_micro * seq_len),
        out_shape=(
            jax.ShapeDtypeStruct((2, n_data, n_micro, *act_shape), BF),
            jax.ShapeDtypeStruct((2, n_micro, seq_len, d_ff), F32),
            jax.ShapeDtypeStruct((n_micro, *act_shape), BF),
            jax.ShapeDtypeStruct((seq_len, 128), F32),
        ),
        in_specs=[hbm] * 4,
        out_specs=(hbm, hbm, hbm, pl.BlockSpec(memory_space=pltpu.VMEM)),
        scratch_shapes=[
            pltpu.VMEM((2, d_model, d_ff), BF),
            pltpu.VMEM((2, d_ff, d_model), BF),
            pltpu.VMEM((n_slots, *act_shape), BF),
            pltpu.VMEM((n_slots, *act_shape), BF),
            pltpu.VMEM((seq_len, d_ff), BF),
            pltpu.VMEM((2, seq_len, d_ff), F32),
            pltpu.VMEM((n_micro, *act_shape), BF),
            pltpu.VMEM((n_micro, *act_shape), BF),
            pltpu.VMEM((seq_len, 128), F32),
            dma((2, 4)), dma((2, 2)), dma((n_micro,)), dma, dma((2,)), dma, dma((n_slots,)), dma((n_slots,)),
            *spread_sems(n_slots),
        ],
        compiler_params=pltpu.CompilerParams(collective_id=0, has_side_effects=True, vmem_limit_bytes=VMEM_BYTES),
        name="fwd_pipe",
    )(tokens, targets, up, down)


def bwd_kernel(
    n_stage, top_ref, slope_ref, up_ref, down_ref, gg_ref,
    w_up, w_down, g_in, g_out, d_pre, slope,
    up_sem, down_sem, top_sem, slope_sem, zsend_sem, zrecv_sem, *spread,
):
    n_micro = top_ref.shape[0]
    n_slots = 2 * n_micro
    d_model, d_ff = w_up.shape[1:]
    up_rows = d_model // up_sem.shape[1]
    down_rows = d_ff // down_sem.shape[1]
    place = Place(n_stage)
    is_first = place.stage == 0
    is_last = place.stage == n_stage - 1

    def load_top(i):
        return pltpu.make_async_copy(top_ref.at[i], g_in.at[i], top_sem.at[i])

    def load_up(v, c):
        rows = pl.ds(c * up_rows, up_rows)
        return pltpu.make_async_copy(up_ref.at[v, 0, rows], w_up.at[v, rows], up_sem.at[v, c])

    def load_down(v, c):
        rows = pl.ds(c * down_rows, down_rows)
        return pltpu.make_async_copy(down_ref.at[v, 0, rows], w_down.at[v, rows], down_sem.at[v, c])

    def load_slope(slot):
        v, i, b = 1 - lax.div(slot, n_micro), lax.rem(slot, n_micro), lax.rem(slot, 2)
        return pltpu.make_async_copy(slope_ref.at[v, i], slope.at[b], slope_sem.at[b])

    @pl.when(is_last)
    def _():
        for i in range(n_micro):
            load_top(i).start()

    for v in (1, 0):
        for c in range(down_sem.shape[1]):
            load_down(v, c).start()
            if v == 1 and c == 0:
                load_slope(0).start()
                load_slope(1).start()
        for c in range(up_sem.shape[1]):
            load_up(v, c).start()
    place.barrier()
    gather = Spread(place, g_in, gg_ref, n_micro, spread)

    def hand_on(slot):
        to = slot + n_micro * lax.div(n_stage - 1 - place.stage, n_stage - 1)
        return remote(
            g_out.at[slot], g_in.at[to], zsend_sem.at[slot], zrecv_sem.at[to], place.at(place.prev, place.data)
        )

    def arrive(slot):
        return remote(
            g_out.at[slot], g_in.at[slot], zsend_sem.at[slot], zrecv_sem.at[slot], place.at(place.prev, place.data)
        )

    def body(slot, carry):
        v, i, b = 1 - lax.div(slot, n_micro), lax.rem(slot, n_micro), lax.rem(slot, 2)
        from_top = jnp.logical_and(is_last, v == 1)
        has_next = jnp.logical_not(jnp.logical_and(is_first, v == 0))

        @pl.when(from_top)
        def _():
            load_top(i).wait()

        @pl.when(jnp.logical_not(from_top))
        def _():
            arrive(slot).wait_recv()

        gather.send(slot)

        @pl.when(i == 0)
        def _():
            for c in range(down_sem.shape[1]):
                load_down(v, c).wait()
            for c in range(up_sem.shape[1]):
                load_up(v, c).wait()

        load_slope(slot).wait()

        @pl.when(has_next)
        def _():
            for c in range(down_sem.shape[1]):
                cols = slice(c * down_rows, (c + 1) * down_rows)
                d_act = matmul(g_in[slot], w_down[v, cols, :], ((1,), (1,))).astype(BF)
                d_pre[:, cols] = (slope[b, :, cols] * d_act.astype(F32)).astype(BF)
            for c in range(up_sem.shape[1]):
                cols = slice(c * up_rows, (c + 1) * up_rows)
                back = matmul(d_pre[...], w_up[v, cols, :], ((1,), (1,)))
                g_out[slot, :, cols] = (g_in[slot, :, cols].astype(F32) + back).astype(BF)
            hand_on(slot).start()

        @pl.when(slot < n_slots - 2)
        def _():
            load_slope(slot + 2).start()

        @pl.when(slot >= 2)
        def _():
            gather.forward(slot - 2)

        return carry

    lax.fori_loop(0, n_slots, body, 0)
    gather.forward(n_slots - 2)
    gather.forward(n_slots - 1)
    gather.finish(n_slots)
    n_sent = n_slots - n_micro * lax.div(n_stage - 1 - place.stage, n_stage - 1)

    def drain(slot, carry):
        hand_on(slot).wait_send()
        return carry

    lax.fori_loop(0, n_sent, drain, 0)


def backward(n_stage, n_data, tops, slope, up, down):
    n_micro, seq_len, d_model = tops.shape
    d_ff = up.shape[3]
    n_slots = 2 * n_micro
    dma = pltpu.SemaphoreType.DMA
    hbm = pl.BlockSpec(memory_space=pl.ANY)
    act_shape = (seq_len, d_model)
    return pl.pallas_call(
        functools.partial(bwd_kernel, n_stage),
        out_shape=jax.ShapeDtypeStruct((2, n_data, n_micro, *act_shape), BF),
        in_specs=[hbm] * 4,
        out_specs=hbm,
        scratch_shapes=[
            pltpu.VMEM((2, d_model, d_ff), BF),
            pltpu.VMEM((2, d_ff, d_model), BF),
            pltpu.VMEM((n_slots, *act_shape), BF),
            pltpu.VMEM((n_slots, *act_shape), BF),
            pltpu.VMEM((seq_len, d_ff), BF),
            pltpu.VMEM((2, seq_len, d_ff), F32),
            dma((2, 2)), dma((2, 4)), dma((n_micro,)), dma((2,)), dma((n_slots,)), dma((n_slots,)),
            *spread_sems(n_slots),
        ],
        compiler_params=pltpu.CompilerParams(collective_id=1, has_side_effects=True, vmem_limit_bytes=VMEM_BYTES),
        name="bwd_pipe",
    )(tops, slope, up, down)


def act_bwd(h_in, grad_out, w_one, w_two):
    act_val, gelu_vjp = jax.vjp(gelu_fn, matmul(h_in, w_one, ((1,), (0,))))
    d_act = matmul(grad_out, w_two, ((1,), (1,))).astype(BF)
    d_pre = gelu_vjp(d_act.astype(F32))[0].astype(BF)
    return act_val.astype(BF), d_pre


def solution(mesh):
    n_stage = mesh.shape["stage"]
    n_data = mesh.shape["data"]

    def device_fn(tokens_loc, targets_loc, up_loc, down_loc):
        n_micro, seq_len, d_model = tokens_loc.shape
        d_ff = up_loc.shape[3]
        n_tok = n_data * n_micro * seq_len
        data_idx = lax.axis_index("data")
        h_all, slope, tops, loss = forward(n_stage, n_data, tokens_loc, targets_loc, up_loc, down_loc)
        g_all = backward(n_stage, n_data, tops, slope, up_loc, down_loc)
        f_loc = d_ff // n_data
        ups, downs = [], []
        for virt in range(2):
            h_one = h_all[virt].reshape(-1, d_model)
            g_one = g_all[1 - virt].reshape(-1, d_model)
            w_one = lax.dynamic_slice(up_loc[virt, 0], (0, data_idx * f_loc), (d_model, f_loc))
            w_two = lax.dynamic_slice(down_loc[virt, 0], (data_idx * f_loc, 0), (f_loc, d_model))
            act, d_pre = act_bwd(h_one, g_one, w_one, w_two)
            downs.append(matmul(act, g_one, ((0,), (0,))))
            g_up = matmul(h_one, d_pre, ((0,), (0,)))
            ups.append(lax.all_to_all(g_up, "data", 0, 1, tiled=True))
        loss = lax.psum(jnp.sum(loss) / (2.0 * n_tok), ("stage", "data"))
        return loss, jnp.stack(ups)[:, None], jnp.stack(downs)[:, None]

    return jax.shard_map(
        device_fn,
        mesh=mesh,
        in_specs=(P("data"), P("data"), P(None, "stage"), P(None, "stage")),
        out_specs=(P(), P(None, "stage", "data"), P(None, "stage", "data")),
        check_vma=False,
    )
```

```python
import functools

import jax
import jax.numpy as jnp
import numpy as np
from jax import lax
from jax.experimental import pallas as pl
from jax.experimental.pallas import tpu as pltpu
from jax.sharding import PartitionSpec as P

BF = jnp.bfloat16
F32 = jnp.float32
MESH = pl.DeviceIdType.MESH
VMEM_BYTES = 67043328


def gelu_fn(pre_act):
    return jax.nn.gelu(pre_act, approximate=True)


def gelu_and_slope(pre_act):
    c_one, c_two = np.float32(np.sqrt(2.0 / np.pi)), np.float32(0.044715)
    square = pre_act * pre_act
    tanh = jnp.tanh(c_one * (pre_act + c_two * (square * pre_act)))
    cdf = 0.5 * (1.0 + tanh)
    inner = c_one + (c_one * 3 * c_two) * square
    return pre_act * cdf, cdf + (0.5 * pre_act) * ((1.0 - tanh * tanh) * inner)


def matmul(lhs, rhs, dims):
    return lax.dot_general(lhs, rhs, (dims, ((), ())), preferred_element_type=F32)


class Place:
    def __init__(self, n_stage):
        self.stage = lax.axis_index("stage")
        self.data = lax.axis_index("data")
        core = lax.rem(self.data, 2)
        x = lax.rem(lax.div(self.data, 2), 2)
        y = lax.div(self.data, 4)
        self.partner = self.data + 1 - 2 * core
        dx, dy = 2 - 4 * x, 4 - 8 * y
        self.moves = (dx, dy, dx + dy)
        self.next = lax.rem(self.stage + 1, n_stage)
        self.prev = lax.rem(self.stage + n_stage - 1, n_stage)

    def at(self, stage, data):
        return {"stage": stage, "data": data}

    def peers(self):
        yield self.at(self.next, self.data)
        yield self.at(self.prev, self.data)
        yield self.at(self.stage, self.partner)
        for move in self.moves:
            yield self.at(self.stage, self.data + move)

    def barrier(self):
        sem = pltpu.get_barrier_semaphore()
        for peer in self.peers():
            pl.semaphore_signal(sem, inc=1, device_id=peer, device_id_type=MESH)
        pl.semaphore_wait(sem, 6)


def remote(src, dst, send_sem, recv_sem, device):
    return pltpu.make_async_remote_copy(
        src_ref=src, dst_ref=dst, send_sem=send_sem, recv_sem=recv_sem, device_id=device, device_id_type=MESH
    )


class Spread:
    def __init__(self, place, src, dst, n_micro, sems):
        self.place, self.src, self.dst, self.n_micro = place, src, dst, n_micro
        self.own_sem, self.send_sem, self.recv_sem, self.fsend_sem, self.frecv_sem = sems

    def spot(self, slot, data):
        return self.dst.at[lax.div(slot, self.n_micro), data, lax.rem(slot, self.n_micro)]

    def own(self, slot):
        return pltpu.make_async_copy(self.src.at[slot], self.spot(slot, self.place.data), self.own_sem.at[slot])

    def direct(self, slot, k):
        place = self.place
        peer = place.partner if k == 0 else place.data + place.moves[k - 1]
        return remote(
            self.src.at[slot],
            self.spot(slot, place.data),
            self.send_sem.at[slot, k],
            self.recv_sem.at[slot, k],
            place.at(place.stage, peer),
        )

    def relay(self, slot, k):
        place = self.place
        spot = self.spot(slot, place.data + place.moves[k])
        return remote(
            spot, spot, self.fsend_sem.at[slot, k], self.frecv_sem.at[slot, k], place.at(place.stage, place.partner)
        )

    def send(self, slot):
        self.own(slot).start()
        for k in range(4):
            self.direct(slot, k).start()

    def forward(self, slot):
        for k in range(3):
            self.direct(slot, k + 1).wait_recv()
            self.relay(slot, k).start()

    def finish(self, n_slots):
        def body(slot, carry):
            self.own(slot).wait()
            self.direct(slot, 0).wait_recv()
            for k in range(4):
                self.direct(slot, k).wait_send()
            for k in range(3):
                self.relay(slot, k).wait()
            return carry

        lax.fori_loop(0, n_slots, body, 0)


def spread_sems(n_slots):
    dma = pltpu.SemaphoreType.DMA
    return [dma((n_slots,)), dma((n_slots, 4)), dma((n_slots, 4)), dma((n_slots, 3)), dma((n_slots, 3))]


def fwd_kernel(
    n_stage, n_tok, tok_ref, tgt_ref, up_ref, down_ref, hg_ref, slope_ref, top_ref, loss_ref,
    w_up, w_down, h_in, h_out, act, slope, tgt, top, loss,
    up_sem, down_sem, tok_sem, tgt_sem, slope_sem, top_sem, zsend_sem, zrecv_sem, *spread,
):
    n_micro = tok_ref.shape[0]
    n_slots = 2 * n_micro
    d_model, d_ff = w_up.shape[1:]
    up_cols = d_ff // up_sem.shape[1]
    down_cols = d_model // down_sem.shape[1]
    place = Place(n_stage)
    is_first = place.stage == 0
    is_last = place.stage == n_stage - 1

    def load_tok(i):
        return pltpu.make_async_copy(tok_ref.at[i], h_in.at[i], tok_sem.at[i])

    def load_up(v, c):
        cols = pl.ds(c * up_cols, up_cols)
        return pltpu.make_async_copy(up_ref.at[v, 0, :, cols], w_up.at[v, :, cols], up_sem.at[v, c])

    def load_down(v, c):
        cols = pl.ds(c * down_cols, down_cols)
        return pltpu.make_async_copy(down_ref.at[v, 0, :, cols], w_down.at[v, :, cols], down_sem.at[v, c])

    @pl.when(is_first)
    def _():
        for i in range(n_micro):
            load_tok(i).start()

    for v in range(2):
        for c in range(up_sem.shape[1]):
            load_up(v, c).start()
        for c in range(down_sem.shape[1]):
            load_down(v, c).start()
    load_tgt = pltpu.make_async_copy(tgt_ref, tgt, tgt_sem)
    load_tgt.start()
    loss[...] = jnp.zeros_like(loss)
    place.barrier()
    gather = Spread(place, h_in, hg_ref, n_micro, spread)

    def put_slope(slot):
        v, i, b = lax.div(slot, n_micro), lax.rem(slot, n_micro), lax.rem(slot, 2)
        return pltpu.make_async_copy(slope.at[b], slope_ref.at[v, i], slope_sem.at[b])

    def hand_on(slot):
        to = slot + n_micro * lax.div(place.stage, n_stage - 1)
        return remote(
            h_out.at[slot], h_in.at[to], zsend_sem.at[slot], zrecv_sem.at[to], place.at(place.next, place.data)
        )

    def arrive(slot):
        return remote(
            h_out.at[slot], h_in.at[slot], zsend_sem.at[slot], zrecv_sem.at[slot], place.at(place.next, place.data)
        )

    def body(slot, carry):
        v, i, b = lax.div(slot, n_micro), lax.rem(slot, n_micro), lax.rem(slot, 2)
        from_data = jnp.logical_and(is_first, v == 0)
        is_top = jnp.logical_and(is_last, v == 1)

        @pl.when(from_data)
        def _():
            load_tok(i).wait()

        @pl.when(jnp.logical_not(from_data))
        def _():
            arrive(slot).wait_recv()

        gather.send(slot)

        @pl.when(i == 0)
        def _():
            for c in range(up_sem.shape[1]):
                load_up(v, c).wait()

        @pl.when(slot >= 2)
        def _():
            put_slope(slot - 2).wait()

        for c in range(up_sem.shape[1]):
            cols = slice(c * up_cols, (c + 1) * up_cols)
            pre_act = matmul(h_in[slot], w_up[v, :, cols], ((1,), (0,)))
            act_val, slope_val = gelu_and_slope(pre_act)
            act[:, cols] = act_val.astype(BF)
            slope[b, :, cols] = slope_val
        put_slope(slot).start()

        @pl.when(i == 0)
        def _():
            for c in range(down_sem.shape[1]):
                load_down(v, c).wait()

        for c in range(down_sem.shape[1]):
            cols = slice(c * down_cols, (c + 1) * down_cols)
            out_val = matmul(act[...], w_down[v, :, cols], ((1,), (0,)))
            h_out[slot, :, cols] = (h_in[slot, :, cols].astype(F32) + out_val).astype(BF)

        @pl.when(jnp.logical_not(is_top))
        def _():
            hand_on(slot).start()

        @pl.when(is_top)
        def _():
            @pl.when(i == 0)
            def _():
                load_tgt.wait()

            for c in range(d_model // 128):
                cols = slice(c * 128, (c + 1) * 128)
                err = h_out[slot, :, cols].astype(F32) - tgt[i, :, cols].astype(F32)
                loss[...] += err * err
                top[i, :, cols] = (err / n_tok).astype(BF)

        @pl.when(slot >= 2)
        def _():
            gather.forward(slot - 2)

        return carry

    lax.fori_loop(0, n_slots, body, 0)
    loss_ref[...] = loss[...]
    put_top = pltpu.make_async_copy(top, top_ref, top_sem)

    @pl.when(is_last)
    def _():
        put_top.start()

    @pl.when(jnp.logical_not(is_last))
    def _():
        load_tgt.wait()

    gather.forward(n_slots - 2)
    gather.forward(n_slots - 1)
    gather.finish(n_slots)
    put_slope(n_slots - 2).wait()
    put_slope(n_slots - 1).wait()
    n_sent = n_slots - n_micro * lax.div(place.stage, n_stage - 1)

    def drain(slot, carry):
        hand_on(slot).wait_send()
        return carry

    lax.fori_loop(0, n_sent, drain, 0)

    @pl.when(is_last)
    def _():
        put_top.wait()


def forward(n_stage, n_data, tokens, targets, up, down):
    n_micro, seq_len, d_model = tokens.shape
    d_ff = up.shape[3]
    n_slots = 2 * n_micro
    dma = pltpu.SemaphoreType.DMA
    hbm = pl.BlockSpec(memory_space=pl.ANY)
    act_shape = (seq_len, d_model)
    return pl.pallas_call(
        functools.partial(fwd_kernel, n_stage, n_data * n_micro * seq_len),
        out_shape=(
            jax.ShapeDtypeStruct((2, n_data, n_micro, *act_shape), BF),
            jax.ShapeDtypeStruct((2, n_micro, seq_len, d_ff), F32),
            jax.ShapeDtypeStruct((n_micro, *act_shape), BF),
            jax.ShapeDtypeStruct((seq_len, 128), F32),
        ),
        in_specs=[hbm] * 4,
        out_specs=(hbm, hbm, hbm, pl.BlockSpec(memory_space=pltpu.VMEM)),
        scratch_shapes=[
            pltpu.VMEM((2, d_model, d_ff), BF),
            pltpu.VMEM((2, d_ff, d_model), BF),
            pltpu.VMEM((n_slots, *act_shape), BF),
            pltpu.VMEM((n_slots, *act_shape), BF),
            pltpu.VMEM((seq_len, d_ff), BF),
            pltpu.VMEM((2, seq_len, d_ff), F32),
            pltpu.VMEM((n_micro, *act_shape), BF),
            pltpu.VMEM((n_micro, *act_shape), BF),
            pltpu.VMEM((seq_len, 128), F32),
            dma((2, 4)), dma((2, 2)), dma((n_micro,)), dma, dma((2,)), dma, dma((n_slots,)), dma((n_slots,)),
            *spread_sems(n_slots),
        ],
        compiler_params=pltpu.CompilerParams(collective_id=0, has_side_effects=True, vmem_limit_bytes=VMEM_BYTES),
        name="fwd_pipe",
    )(tokens, targets, up, down)


def bwd_kernel(
    n_stage, top_ref, slope_ref, up_ref, down_ref, gg_ref,
    w_up, w_down, g_in, g_out, d_pre, slope,
    up_sem, down_sem, top_sem, slope_sem, zsend_sem, zrecv_sem, *spread,
):
    n_micro = top_ref.shape[0]
    n_slots = 2 * n_micro
    d_model, d_ff = w_up.shape[1:]
    up_rows = d_model // up_sem.shape[1]
    down_rows = d_ff // down_sem.shape[1]
    place = Place(n_stage)
    is_first = place.stage == 0
    is_last = place.stage == n_stage - 1

    def load_top(i):
        return pltpu.make_async_copy(top_ref.at[i], g_in.at[i], top_sem.at[i])

    def load_up(v, c):
        rows = pl.ds(c * up_rows, up_rows)
        return pltpu.make_async_copy(up_ref.at[v, 0, rows], w_up.at[v, rows], up_sem.at[v, c])

    def load_down(v, c):
        rows = pl.ds(c * down_rows, down_rows)
        return pltpu.make_async_copy(down_ref.at[v, 0, rows], w_down.at[v, rows], down_sem.at[v, c])

    def load_slope(slot):
        v, i, b = 1 - lax.div(slot, n_micro), lax.rem(slot, n_micro), lax.rem(slot, 2)
        return pltpu.make_async_copy(slope_ref.at[v, i], slope.at[b], slope_sem.at[b])

    @pl.when(is_last)
    def _():
        for i in range(n_micro):
            load_top(i).start()

    for v in (1, 0):
        for c in range(down_sem.shape[1]):
            load_down(v, c).start()
            if v == 1 and c == 0:
                load_slope(0).start()
                load_slope(1).start()
        for c in range(up_sem.shape[1]):
            load_up(v, c).start()
    place.barrier()
    gather = Spread(place, g_in, gg_ref, n_micro, spread)

    def hand_on(slot):
        to = slot + n_micro * lax.div(n_stage - 1 - place.stage, n_stage - 1)
        return remote(
            g_out.at[slot], g_in.at[to], zsend_sem.at[slot], zrecv_sem.at[to], place.at(place.prev, place.data)
        )

    def arrive(slot):
        return remote(
            g_out.at[slot], g_in.at[slot], zsend_sem.at[slot], zrecv_sem.at[slot], place.at(place.prev, place.data)
        )

    def body(slot, carry):
        v, i, b = 1 - lax.div(slot, n_micro), lax.rem(slot, n_micro), lax.rem(slot, 2)
        from_top = jnp.logical_and(is_last, v == 1)
        has_next = jnp.logical_not(jnp.logical_and(is_first, v == 0))

        @pl.when(from_top)
        def _():
            load_top(i).wait()

        @pl.when(jnp.logical_not(from_top))
        def _():
            arrive(slot).wait_recv()

        gather.send(slot)

        @pl.when(i == 0)
        def _():
            for c in range(down_sem.shape[1]):
                load_down(v, c).wait()
            for c in range(up_sem.shape[1]):
                load_up(v, c).wait()

        load_slope(slot).wait()

        @pl.when(has_next)
        def _():
            for c in range(down_sem.shape[1]):
                cols = slice(c * down_rows, (c + 1) * down_rows)
                d_act = matmul(g_in[slot], w_down[v, cols, :], ((1,), (1,))).astype(BF)
                d_pre[:, cols] = (slope[b, :, cols] * d_act.astype(F32)).astype(BF)
            for c in range(up_sem.shape[1]):
                cols = slice(c * up_rows, (c + 1) * up_rows)
                back = matmul(d_pre[...], w_up[v, cols, :], ((1,), (1,)))
                g_out[slot, :, cols] = (g_in[slot, :, cols].astype(F32) + back).astype(BF)
            hand_on(slot).start()

        @pl.when(slot < n_slots - 2)
        def _():
            load_slope(slot + 2).start()

        @pl.when(slot >= 2)
        def _():
            gather.forward(slot - 2)

        return carry

    lax.fori_loop(0, n_slots, body, 0)
    gather.forward(n_slots - 2)
    gather.forward(n_slots - 1)
    gather.finish(n_slots)
    n_sent = n_slots - n_micro * lax.div(n_stage - 1 - place.stage, n_stage - 1)

    def drain(slot, carry):
        hand_on(slot).wait_send()
        return carry

    lax.fori_loop(0, n_sent, drain, 0)


def backward(n_stage, n_data, tops, slope, up, down):
    n_micro, seq_len, d_model = tops.shape
    d_ff = up.shape[3]
    n_slots = 2 * n_micro
    dma = pltpu.SemaphoreType.DMA
    hbm = pl.BlockSpec(memory_space=pl.ANY)
    act_shape = (seq_len, d_model)
    return pl.pallas_call(
        functools.partial(bwd_kernel, n_stage),
        out_shape=jax.ShapeDtypeStruct((2, n_data, n_micro, *act_shape), BF),
        in_specs=[hbm] * 4,
        out_specs=hbm,
        scratch_shapes=[
            pltpu.VMEM((2, d_model, d_ff), BF),
            pltpu.VMEM((2, d_ff, d_model), BF),
            pltpu.VMEM((n_slots, *act_shape), BF),
            pltpu.VMEM((n_slots, *act_shape), BF),
            pltpu.VMEM((seq_len, d_ff), BF),
            pltpu.VMEM((2, seq_len, d_ff), F32),
            dma((2, 2)), dma((2, 4)), dma((n_micro,)), dma((2,)), dma((n_slots,)), dma((n_slots,)),
            *spread_sems(n_slots),
        ],
        compiler_params=pltpu.CompilerParams(collective_id=1, has_side_effects=True, vmem_limit_bytes=VMEM_BYTES),
        name="bwd_pipe",
    )(tops, slope, up, down)


def wgrad_kernel(
    n_stage, h_ref, g_ref, up_ref, down_ref, part_ref, gup_ref, gdown_ref, loss_ref,
    h_buf, g_buf, w_up, w_down, act, d_pre, d_act, acc_down, acc_a, acc_b, parts,
    h_sem, g_sem, up_sem, down_sem, gd_sem, own_sem, send_sem, recv_sem, csend_sem, crecv_sem, psend_sem, precv_sem,
):
    n_data, n_micro, seq_len, d_model = h_ref.shape[1:]
    f_loc = w_up.shape[3]
    rows = d_model // n_data
    n_tok = n_data * seq_len
    half = d_model // 2
    wide = acc_b.shape[2]
    stage, data = lax.axis_index("stage"), lax.axis_index("data")
    core = lax.rem(data, 2)
    x = lax.rem(lax.div(data, 2), 2)
    y = lax.div(data, 4)
    odd = x + y - 2 * x * y
    dc, dx, dy = 1 - 2 * core, 2 - 4 * x, 4 - 8 * y
    other = data + dx * (1 - odd) + dy * odd
    blocks = (data * (1 - odd) + other * odd, other * (1 - odd) + data * odd)
    plane = (dc, dx, dx + dc, dy, dy + dc, dx + dy, dx + dy + dc)

    def at(stage_idx, data_idx):
        return {"stage": stage_idx, "data": data_idx}

    def column(k):
        return at(lax.rem(stage + k, n_stage), data)

    def block_cols(k):
        return pl.ds(pl.multiple_of(blocks[k] * f_loc, f_loc), f_loc)

    def load_up(v, k):
        return pltpu.make_async_copy(up_ref.at[v, 0, :, block_cols(k)], w_up.at[v, k], up_sem.at[v, k])

    def load_down(v, k):
        return pltpu.make_async_copy(down_ref.at[v, 0, block_cols(k), :], w_down.at[v, k], down_sem.at[v, k])

    def load_h(t):
        v, i, b = 1 - lax.div(t, n_micro), lax.rem(t, n_micro), lax.rem(t, 2)
        return pltpu.make_async_copy(h_ref.at[v, :, i], h_buf.at[b], h_sem.at[b])

    def load_g(t):
        v, i, b = lax.div(t, n_micro), lax.rem(t, n_micro), lax.rem(t, 2)
        return pltpu.make_async_copy(g_ref.at[v, :, i], g_buf.at[b], g_sem.at[b])

    for v in (1, 0):
        for k in range(2):
            load_down(v, k).start()
            load_up(v, k).start()
        if v == 1:
            load_g(0).start()
            load_h(0).start()
            load_g(1).start()
            load_h(1).start()

    sem = pltpu.get_barrier_semaphore()
    for k in range(1, n_stage):
        pl.semaphore_signal(sem, inc=1, device_id=column(k), device_id_type=MESH)
    for move in plane:
        pl.semaphore_signal(sem, inc=1, device_id=at(stage, data + move), device_id_type=MESH)
    pl.semaphore_wait(sem, n_stage - 1 + len(plane))

    is_last = stage == n_stage - 1

    def column_send(k):
        spot = parts.at[data]
        return remote(spot, spot, csend_sem.at[k - 1], crecv_sem, column(k))

    def plane_send(k):
        spot = parts.at[data]
        return remote(spot, spot, psend_sem.at[k], precv_sem.at[k], at(stage, data + plane[k]))

    @pl.when(is_last)
    def _():
        total = part_ref[0:8]
        for k in range(1, seq_len // 8):
            total = total + part_ref[8 * k : 8 * k + 8]
        parts[data] = total

    def store_down(v):
        return pltpu.make_async_copy(acc_down.at[v], gdown_ref.at[v, 0], gd_sem.at[v])

    def pieces(v, kind):
        for there in range(2):
            for flip in range(2):
                to_core = core + flip * dc
                if kind == 0:
                    to = data + flip * dc + there * dx
                    src = acc_a.at[v, pl.ds(pl.multiple_of((to - y * 4) * rows, 8), rows)]
                else:
                    to = data + flip * dc + there * dy
                    first = x * ((2 * rows) % 128) + to_core * rows
                    src = acc_b.at[v, lax.div(to, 4), pl.ds(pl.multiple_of(first, 8), rows)]
                yield src, to, 3 * kind + 2 * there + flip - 1

    def exchange(v, kind):
        for src, to, k in pieces(v, kind):
            dst = gup_ref.at[v, 0, :, block_cols(kind)]
            if k == 3 * kind - 1:
                yield pltpu.make_async_copy(src, dst, own_sem.at[v, kind])
            else:
                yield remote(src, dst, send_sem.at[v, k], recv_sem.at[v, k], at(stage, to))

    def body(t, carry):
        v, i, b = 1 - lax.div(t, n_micro), lax.rem(t, n_micro), lax.rem(t, 2)

        @pl.when(i == 0)
        def _():
            for k in range(2):
                load_down(v, k).wait()
                load_up(v, k).wait()
            acc_down[v] = jnp.zeros(acc_down.shape[1:], F32)
            acc_a[v] = jnp.zeros(acc_a.shape[1:], F32)
            acc_b[v] = jnp.zeros(acc_b.shape[1:], F32)

        load_g(t).wait()
        load_h(t).wait()
        for k in range(2):
            for r in range(2):
                part = slice(r * n_data // 2, (r + 1) * n_data // 2)
                spots = slice(r * n_tok // 2, (r + 1) * n_tok // 2)
                g_part = g_buf[b, part].reshape(-1, d_model)
                h_part = h_buf[b, part].reshape(-1, d_model)
                d_act[spots] = matmul(g_part, w_down[v, k], ((1,), (1,))).astype(BF)
                act_val, slope_val = gelu_and_slope(matmul(h_part, w_up[v, k], ((1,), (0,))))
                act[k, spots] = act_val.astype(BF)
                d_pre[k, spots] = (slope_val * d_act[spots].astype(F32)).astype(BF)
        a_cols = pl.ds(pl.multiple_of(y * half, half), half)
        acc_a[v] += matmul(h_buf[b, :, :, a_cols].reshape(n_tok, half), d_pre[0], ((0,), (0,)))
        for q in range(2):
            first = q * half + x * (2 * rows - (2 * rows) % 128)
            b_cols = pl.ds(pl.multiple_of(first, 128), wide)
            acc_b[v, q] += matmul(h_buf[b, :, :, b_cols].reshape(n_tok, wide), d_pre[1], ((0,), (0,)))

        @pl.when(i == n_micro - 1)
        def _():
            for kind in range(2):
                for copy in exchange(v, kind):
                    copy.start()

        acc_down[v] += matmul(act[odd], g_buf[b].reshape(n_tok, d_model), ((0,), (0,)))

        @pl.when(i == n_micro - 1)
        def _():
            store_down(v).start()

        @pl.when(t < 2 * n_micro - 2)
        def _():
            load_g(t + 2).start()
            load_h(t + 2).start()

        @pl.when(jnp.logical_and(t == 0, is_last))
        def _():
            for k in range(1, n_stage):
                column_send(k).start()

        @pl.when(t == 1)
        def _():
            @pl.when(jnp.logical_not(is_last))
            def _():
                column_send(1).wait_recv()

            for k in range(len(plane)):
                plane_send(k).start()

        return carry

    lax.fori_loop(0, 2 * n_micro, body, 0)

    for k in range(len(plane)):
        plane_send(k).wait()
    total = parts[0]
    for k in range(1, n_data):
        total = total + parts[k]
    loss_ref[...] = total

    @pl.when(is_last)
    def _():
        for k in range(1, n_stage):
            column_send(k).wait_send()

    for v in (1, 0):
        store_down(v).wait()
        for kind in range(2):
            for copy in exchange(v, kind):
                copy.wait()


def weight_grads(n_stage, n_data, h_all, g_all, up, down, loss):
    n_micro, seq_len, d_model = h_all.shape[2:]
    d_ff = up.shape[3]
    f_loc = d_ff // n_data
    n_tok = n_data * seq_len
    wide = -(-(d_model // 4 + (d_model // 4) % 128) // 128) * 128
    dma = pltpu.SemaphoreType.DMA
    hbm = pl.BlockSpec(memory_space=pl.ANY)
    vmem = pl.BlockSpec(memory_space=pltpu.VMEM)
    return pl.pallas_call(
        functools.partial(wgrad_kernel, n_stage),
        out_shape=(
            jax.ShapeDtypeStruct((2, 1, d_model // n_data, d_ff), F32),
            jax.ShapeDtypeStruct((2, 1, f_loc, d_model), F32),
            jax.ShapeDtypeStruct((8, 128), F32),
        ),
        in_specs=[hbm] * 4 + [vmem],
        out_specs=(hbm, hbm, vmem),
        scratch_shapes=[
            pltpu.VMEM((2, n_data, seq_len, d_model), BF),
            pltpu.VMEM((2, n_data, seq_len, d_model), BF),
            pltpu.VMEM((2, 2, d_model, f_loc), BF),
            pltpu.VMEM((2, 2, f_loc, d_model), BF),
            pltpu.VMEM((2, n_tok, f_loc), BF),
            pltpu.VMEM((2, n_tok, f_loc), BF),
            pltpu.VMEM((n_tok, f_loc), BF),
            pltpu.VMEM((2, f_loc, d_model), F32),
            pltpu.VMEM((2, d_model // 2, f_loc), F32),
            pltpu.VMEM((2, 2, wide, f_loc), F32),
            pltpu.VMEM((n_data, 8, 128), F32),
            dma((2,)), dma((2,)), dma((2, 2)), dma((2, 2)), dma((2,)), dma((2, 2)), dma((2, 6)), dma((2, 6)),
            dma((n_stage - 1,)), dma, dma((7,)), dma((7,)),
        ],
        compiler_params=pltpu.CompilerParams(collective_id=2, has_side_effects=True, vmem_limit_bytes=VMEM_BYTES),
        name="wgrad",
    )(h_all, g_all, up, down, loss)


def solution(mesh):
    n_stage = mesh.shape["stage"]
    n_data = mesh.shape["data"]

    def device_fn(tokens_loc, targets_loc, up_loc, down_loc):
        n_micro, seq_len, _ = tokens_loc.shape
        n_tok = n_data * n_micro * seq_len
        h_all, slope, tops, loss = forward(n_stage, n_data, tokens_loc, targets_loc, up_loc, down_loc)
        g_all = backward(n_stage, n_data, tops, slope, up_loc, down_loc)
        grad_up, grad_down, loss = weight_grads(n_stage, n_data, h_all, g_all, up_loc, down_loc, loss)
        return jnp.sum(loss) / (2.0 * n_tok), grad_up, grad_down

    return jax.shard_map(
        device_fn,
        mesh=mesh,
        in_specs=(P("data"), P("data"), P(None, "stage"), P(None, "stage")),
        out_specs=(P(), P(None, "stage", "data"), P(None, "stage", "data")),
        check_vma=False,
    )
```

```python
import functools

import jax
import jax.numpy as jnp
import numpy as np
from jax import lax
from jax.experimental import pallas as pl
from jax.experimental.pallas import tpu as pltpu
from jax.sharding import PartitionSpec as P

BF = jnp.bfloat16
F32 = jnp.float32
MESH = pl.DeviceIdType.MESH
VMEM_BYTES = 67043328
NN, NT, TN = ((1,), (0,)), ((1,), (1,)), ((0,), (0,))


def matmul(lhs, rhs, dims):
    return lax.dot_general(lhs, rhs, (dims, ((), ())), preferred_element_type=F32)


def gelu_and_slope(pre_act):
    c_one, c_two = np.float32(np.sqrt(2.0 / np.pi)), np.float32(0.044715)
    square = pre_act * pre_act
    tanh = jnp.tanh(c_one * (pre_act + c_two * (square * pre_act)))
    cdf = 0.5 * (1.0 + tanh)
    inner = c_one + (c_one * 3 * c_two) * square
    return pre_act * cdf, cdf + (0.5 * pre_act) * ((1.0 - tanh * tanh) * inner)


def local(src, dst, sem):
    return pltpu.make_async_copy(src, dst, sem)


def remote(src, dst, send_sem, recv_sem, device):
    return pltpu.make_async_remote_copy(
        src_ref=src, dst_ref=dst, send_sem=send_sem, recv_sem=recv_sem, device_id=device, device_id_type=MESH
    )


def ds(start, size):
    return pl.ds(start if isinstance(start, int) else pl.multiple_of(start, size), size)


def when(*terms):
    cond = terms[0]
    for term in terms[1:]:
        cond = jnp.logical_and(cond, term)
    return pl.when(cond)


class Place:
    def __init__(self, n_stage):
        self.n_stage = n_stage
        self.stage = stage = lax.axis_index("stage")
        self.data = data = lax.axis_index("data")
        self.core = lax.rem(data, 2)
        self.x = lax.rem(lax.div(data, 2), 2)
        self.y = lax.div(data, 4)
        self.dc, self.dx, self.dy = 1 - 2 * self.core, 2 - 4 * self.x, 4 - 8 * self.y
        self.odd = self.x + self.y - 2 * self.x * self.y
        self.first = lax.div(n_stage - 1 - stage, n_stage - 1)
        self.last = lax.div(stage, n_stage - 1)
        self.is_first = stage == 0
        self.is_last = stage == n_stage - 1
        self.plane = (self.dc, self.dx, self.dx + self.dc, self.dy, self.dy + self.dc)
        self.plane += (self.dx + self.dy, self.dx + self.dy + self.dc)

    def peer(self, move):
        return {"stage": self.stage, "data": self.data + move}

    def column(self, k):
        return {"stage": lax.rem(self.stage + k, self.n_stage), "data": self.data}

    def barrier(self):
        sem = pltpu.get_barrier_semaphore()
        peers = [self.column(k) for k in range(1, self.n_stage)] + [self.peer(move) for move in self.plane]
        for peer in peers:
            pl.semaphore_signal(sem, inc=1, device_id=peer, device_id_type=MESH)
        pl.semaphore_wait(sem, len(peers))


class Spread:
    def __init__(self, place, src, dst, n_micro, sems):
        self.place, self.src, self.dst, self.n_micro = place, src, dst, n_micro
        self.moves = (place.dx, place.dy, place.dx + place.dy)
        self.own_sem, self.send_sem, self.recv_sem, self.fsend_sem, self.frecv_sem = sems

    def spot(self, slot, data):
        rows = ds(data * self.src.shape[1], self.src.shape[1])
        return self.dst.at[lax.div(slot, self.n_micro), lax.rem(slot, self.n_micro), rows]

    def own(self, slot):
        return local(self.src.at[slot], self.spot(slot, self.place.data), self.own_sem.at[slot])

    def direct(self, slot, k):
        move = self.place.dc if k == 0 else self.moves[k - 1]
        spot = self.spot(slot, self.place.data)
        return remote(
            self.src.at[slot], spot, self.send_sem.at[slot, k], self.recv_sem.at[slot, k], self.place.peer(move)
        )

    def relay(self, slot, k):
        spot = self.spot(slot, self.place.data + self.moves[k])
        return remote(
            spot, spot, self.fsend_sem.at[slot, k], self.frecv_sem.at[slot, k], self.place.peer(self.place.dc)
        )

    def send(self, slot):
        self.own(slot).start()
        for k in range(4):
            self.direct(slot, k).start()

    def forward(self, slot):
        for k in range(3):
            self.direct(slot, k + 1).wait_recv()
            self.relay(slot, k).start()

    def sent(self, slot):
        self.own(slot).wait()
        for k in range(4):
            self.direct(slot, k).wait_send()

    def ready(self, slot):
        self.direct(slot, 0).wait_recv()
        for k in range(3):
            self.relay(slot, k).wait_recv()

    def drain(self, n_slots):
        def body(slot, carry):
            for k in range(3):
                self.relay(slot, k).wait_send()
            return carry

        lax.fori_loop(0, n_slots, body, 0)


def kernel(
    n_stage, pieces, tok_ref, tgt_ref, up_ref, down_ref, gup_ref, gdown_ref, loss_ref, hg_ref, gg_ref, slope_ref,
    w_up, w_down, held, out, mid, slope, sq_err, parts, acc_down, acc_a, acc_b,
    up_sem, down_sem, tok_sem, tgt_sem, slope_sem, fsend_sem, frecv_sem, bsend_sem, brecv_sem,
    wu_sem, wd_sem, hbuf_sem, gbuf_sem, gd_sem, own_sem, xsend_sem, xrecv_sem, csend_sem, crecv_sem, psend_sem, precv_sem,
    *spread,
):
    n_micro, seq_len, d_model = tok_ref.shape
    n_data = hg_ref.shape[2] // seq_len
    n_slots = 2 * n_micro
    d_ff = up_ref.shape[3]
    f_loc = d_ff // n_data
    rows = d_model // n_data
    half = d_model // 2
    wide = acc_b.shape[1]
    n_chunk = n_data * seq_len
    n_tok = n_micro * n_chunk
    n_up, n_down = up_sem.shape[1], down_sem.shape[1]
    up_cols, down_cols = d_ff // n_up, d_model // n_down
    place = Place(n_stage)
    first, is_first, is_last, odd = place.first, place.is_first, place.is_last, place.odd


    def load_tok(i):
        return local(tok_ref.at[i], held.at[i], tok_sem.at[i])

    def load_up(v, c):
        cols = pl.ds(c * up_cols, up_cols)
        return local(up_ref.at[v, 0, :, cols], w_up.at[v, :, cols], up_sem.at[v, c])

    def load_down(v, c):
        cols = pl.ds(c * down_cols, down_cols)
        return local(down_ref.at[v, 0, :, cols], w_down.at[v, :, cols], down_sem.at[v, c])

    def load_tgt(i):
        return local(tgt_ref.at[i], held.at[i], tgt_sem)

    @when(is_first)
    def _():
        for i in range(n_micro):
            load_tok(i).start()

    for v in range(2):
        for c in range(n_up):
            load_up(v, c).start()
        for c in range(n_down):
            load_down(v, c).start()

    sq_err[...] = jnp.zeros_like(sq_err)
    place.barrier()
    gather_h = Spread(place, held, hg_ref, n_micro, spread[:5])
    gather_g = Spread(place, held, gg_ref, n_micro, spread[5:])

    def put_slope(slot):
        v, i, b = lax.div(slot, n_micro), lax.rem(slot, n_micro), lax.rem(slot, 2)
        return local(slope.at[b], slope_ref.at[v, i], slope_sem.at[b])

    def fwd_piece(slot, cols):
        to = slot + n_micro * place.last
        src = out.at[lax.rem(slot, 2), :, cols]
        return remote(src, held.at[to, :, cols], fsend_sem.at[slot], frecv_sem.at[to], place.column(1))

    def fwd_whole(slot):
        src = out.at[lax.rem(slot, 2)]
        return remote(src, held.at[slot], fsend_sem.at[slot], frecv_sem.at[slot], place.column(1))

    def fwd_slot(slot, carry):
        v, i, b = lax.div(slot, n_micro), lax.rem(slot, n_micro), lax.rem(slot, 2)
        from_data = jnp.logical_and(is_first, v == 0)
        is_top = jnp.logical_and(is_last, v == 1)

        @when(from_data)
        def _():
            load_tok(i).wait()

        @when(jnp.logical_not(from_data))
        def _():
            fwd_whole(slot).wait_recv()

        gather_h.send(slot)

        @when(v == 1)
        def _():
            gather_h.sent(slot - n_micro)

            @when(is_last)
            def _():
                load_tgt(i).start()

        @when(i == 0)
        def _():
            for c in range(n_up):
                load_up(v, c).wait()

        @when(slot >= 2)
        def _():
            put_slope(slot - 2).wait()

        for c in range(n_up):
            cols = slice(c * up_cols, (c + 1) * up_cols)
            act_val, slope_val = gelu_and_slope(matmul(held[slot], w_up[v, :, cols], NN))
            mid[:, cols] = act_val.astype(BF)
            slope[b, :, cols] = slope_val
        put_slope(slot).start()

        @when(i == 0)
        def _():
            for c in range(n_down):
                load_down(v, c).wait()

        @when(slot >= 2, jnp.logical_not(jnp.logical_and(is_last, slot >= n_micro + 2)))
        def _():
            fwd_whole(slot - 2).wait_send()

        for start, size in pieces:
            cols = slice(start, start + size)
            out_val = matmul(mid[...], w_down[v, :, cols], NN)
            out[b, :, cols] = (held[slot, :, cols].astype(F32) + out_val).astype(BF)

            @when(jnp.logical_not(is_top))
            def _():
                fwd_piece(slot, pl.ds(start, size)).start()

        @when(is_top)
        def _():
            load_tgt(i).wait()
            for c in range(d_model // 128):
                cols = slice(c * 128, (c + 1) * 128)
                err = out[b, :, cols].astype(F32) - held[i, :, cols].astype(F32)
                sq_err[...] += err * err
                held[i, :, cols] = (err / n_tok).astype(BF)

        @when(slot >= 2)
        def _():
            gather_h.forward(slot - 2)

        return carry

    lax.fori_loop(0, n_slots, fwd_slot, 0)

    def column_send(k):
        spot = parts.at[place.data]
        return remote(spot, spot, csend_sem.at[k - 1], crecv_sem, place.column(k))

    def plane_send(k):
        spot = parts.at[place.data]
        return remote(spot, spot, psend_sem.at[k], precv_sem.at[k], place.peer(place.plane[k]))

    @when(is_last)
    def _():
        total = sq_err[0:8]
        for k in range(1, seq_len // 8):
            total = total + sq_err[8 * k : 8 * k + 8]
        parts[place.data] = total


    def load_slope(slot):
        v, i, b = 1 - lax.div(slot, n_micro), lax.rem(slot, n_micro), lax.rem(slot, 2)
        return local(slope_ref.at[v, i], slope.at[b], slope_sem.at[b])

    for slot in range(2):
        put_slope(n_slots - 2 + slot).wait()
        load_slope(slot).start()

    def bwd_piece(slot, cols):
        to = slot + n_micro * first
        src = out.at[lax.rem(slot, 2), :, cols]
        return remote(src, held.at[to, :, cols], bsend_sem.at[slot], brecv_sem.at[to], place.column(n_stage - 1))

    def bwd_whole(slot):
        src = out.at[lax.rem(slot, 2)]
        return remote(src, held.at[slot], bsend_sem.at[slot], brecv_sem.at[slot], place.column(n_stage - 1))

    def bwd_slot(slot):
        p, i, b = lax.div(slot, n_micro), lax.rem(slot, n_micro), lax.rem(slot, 2)
        v = 1 - p

        @when(jnp.logical_not(jnp.logical_and(is_last, p == 0)))
        def _():
            bwd_whole(slot).wait_recv()

        gather_g.send(slot)

        @when(jnp.logical_not(jnp.logical_and(is_first, p == 1)))
        def _():
            load_slope(slot).wait()
            for c in range(n_up):
                cols = slice(c * up_cols, (c + 1) * up_cols)
                d_act = matmul(held[slot], w_down[v, cols, :], NT).astype(BF)
                mid[:, cols] = (slope[b, :, cols] * d_act.astype(F32)).astype(BF)

            @when(p == 0)
            def _():
                gather_h.sent(slot + n_micro)

            @when(slot >= 2)
            def _():
                bwd_whole(slot - 2).wait_send()

            @when(slot < 2, jnp.logical_not(is_last))
            def _():
                fwd_whole(n_slots - 2 + slot).wait_send()

            for start, size in pieces:
                cols = slice(start, start + size)
                back = matmul(mid[...], w_up[v, cols, :], NT)
                out[b, :, cols] = (held[slot, :, cols].astype(F32) + back).astype(BF)
                bwd_piece(slot, pl.ds(start, size)).start()

            @when(i < n_micro - 2)
            def _():
                load_slope(slot + 2).start()


    other = place.data + place.dx * (1 - odd) + place.dy * odd
    blocks = (place.data * (1 - odd) + other * odd, other * (1 - odd) + place.data * odd)

    def wd_rows(p, k):
        return pl.ds(pl.multiple_of(p * (2 * f_loc + 4 * n_chunk) + k * f_loc, 128), f_loc)

    def wu_cols(p, k):
        return pl.ds(pl.multiple_of((5 * p + k) * f_loc, 128), f_loc)

    def buf_rows(n, k):
        return pl.ds(pl.multiple_of(2 * f_loc + (2 * k + lax.rem(n, 2)) * n_chunk, 128), n_chunk)

    def act_cols(k):
        return pl.ds(pl.multiple_of((2 + k) * f_loc, 128), f_loc)

    def block_cols(k):
        return ds(blocks[k] * f_loc, f_loc)

    def load_wu(p, k):
        return local(up_ref.at[1 - p, 0, :, block_cols(k)], w_up.at[1, :, wu_cols(p, k)], wu_sem.at[p, k])

    def load_wd(p, k):
        return local(down_ref.at[1 - p, 0, block_cols(k), :], w_down.at[1, wd_rows(p, k), :], wd_sem.at[p, k])

    def load_h(n):
        p, c, b = lax.div(n, n_micro), lax.rem(n, n_micro), lax.rem(n, 2)
        return local(hg_ref.at[1 - p, c], w_down.at[1, buf_rows(n, 0), :], hbuf_sem.at[b])

    def load_g(n):
        p, c, b = lax.div(n, n_micro), lax.rem(n, n_micro), lax.rem(n, 2)
        return local(gg_ref.at[p, c], w_down.at[1, buf_rows(n, 1), :], gbuf_sem.at[b])

    def h_ready(n):
        p, c = lax.div(n, n_micro), lax.rem(n, n_micro)
        gather_h.ready((1 - p) * n_micro + c)

    def store_down(v):
        return local(acc_down, gdown_ref.at[v, 0], gd_sem)

    def exchange(v, kind):
        for there in range(2):
            for flip in range(2):
                k = 3 * kind + 2 * there + flip - 1
                move = flip * place.dc + there * (place.dx if kind == 0 else place.dy)
                to = place.data + move
                if kind == 0:
                    src = acc_a.at[pl.ds(pl.multiple_of((to - place.y * 4) * rows, 8), rows)]
                else:
                    start = place.x * ((2 * rows) % 128) + lax.rem(to, 2) * rows
                    src = acc_b.at[lax.div(to, 4), pl.ds(pl.multiple_of(start, 8), rows)]
                dst = gup_ref.at[v, 0, :, block_cols(kind)]
                if there == flip == 0:
                    yield functools.partial(local, src, dst, own_sem.at[v, kind])
                else:
                    yield functools.partial(remote, src, dst, xsend_sem.at[v, k], xrecv_sem.at[v, k], place.peer(move))

    def wait_sent(v):
        for kind in range(2):
            for k, copy in enumerate(exchange(v, kind)):
                if k == 0:
                    copy().wait()
                else:
                    copy().wait_send()
        store_down(v).wait()

    def chunk(n):
        p, c = lax.div(n, n_micro), lax.rem(n, n_micro)
        v = 1 - p
        h_rows, g_rows = buf_rows(n, 0), buf_rows(n, 1)
        gather_g.own(n).wait()
        gather_g.ready(n)
        load_g(n).start()

        @when(n < n_slots - 1)
        def _():
            h_ready(n + 1)
            load_h(n + 1).start()

        @when(c == 0)
        def _():
            for k in range(2):
                load_wu(p, k).wait()
                load_wd(p, k).wait()

            @when(p == 1)
            def _():
                wait_sent(1)

            acc_down[...] = jnp.zeros(acc_down.shape, F32)
            acc_a[...] = jnp.zeros(acc_a.shape, F32)
            acc_b[...] = jnp.zeros(acc_b.shape, F32)

        load_h(n).wait()
        part = n_chunk // 2
        for k in range(2):
            for r in range(2):
                spots = pl.ds(r * part, part)
                h_part = w_down[1, pl.ds(pl.multiple_of(h_rows.start + r * part, 64), part), :]
                act_val, slope_val = gelu_and_slope(matmul(h_part, w_up[1, :, wu_cols(p, k)], NN))
                w_up[1, spots, act_cols(k)] = act_val.astype(BF)
                for j in range(n_data // 2):
                    cols = slice((r * n_data // 2 + j) * f_loc, (r * n_data // 2 + j + 1) * f_loc)
                    slope[k, :, cols] = slope_val[j * seq_len : (j + 1) * seq_len]
        load_g(n).wait()
        for k in range(2):
            for r in range(2):
                g_part = w_down[1, pl.ds(pl.multiple_of(g_rows.start + r * part, 64), part), :]
                d_act = matmul(g_part, w_down[1, wd_rows(p, k), :], NT).astype(BF).astype(F32)
                for j in range(n_data // 2):
                    cols = slice((r * n_data // 2 + j) * f_loc, (r * n_data // 2 + j + 1) * f_loc)
                    d_pre = slope[k, :, cols] * d_act[j * seq_len : (j + 1) * seq_len]
                    spots = pl.ds(n_chunk + r * part + j * seq_len, seq_len)
                    w_up[1, spots, act_cols(k)] = d_pre.astype(BF)

        def d_pre_of(k):
            return w_up[1, pl.ds(n_chunk, n_chunk), act_cols(k)]

        acc_a[...] += matmul(w_down[1, h_rows, ds(place.y * half, half)], d_pre_of(0), TN)
        for q in range(2):
            start = q * half + place.x * (2 * rows - (2 * rows) % 128)
            b_cols = pl.ds(pl.multiple_of(start, 128), wide)
            acc_b[q] += matmul(w_down[1, h_rows, b_cols], d_pre_of(1), TN)

        @when(c == n_micro - 1)
        def _():
            for kind in range(2):
                for copy in exchange(v, kind):
                    copy().start()

        act_own = w_up[1, pl.ds(0, n_chunk), pl.ds(pl.multiple_of((2 + odd) * f_loc, 128), f_loc)]
        acc_down[...] += matmul(act_own, w_down[1, g_rows, :], TN)

        @when(c == n_micro - 1)
        def _():
            store_down(v).start()

    n_steps = 2 * n_micro

    def bwd_step(t, carry):
        p, u = lax.div(t, n_steps), lax.rem(t, n_steps)

        @when(u < n_micro)
        def _():
            bwd_slot(p * n_micro + u)

        @when(t == n_micro - 1)
        def _():
            for q in range(2):
                for k in range(2):
                    load_wu(q, k).start()
                    load_wd(q, k).start()
            h_ready(0)
            load_h(0).start()

        c = u - n_micro + 2 * p * first

        @when(c >= 0, c < n_micro)
        def _():
            chunk(p * n_micro + c)

        f = u - 2 + p * first

        @when(f >= 0, f < n_micro)
        def _():
            gather_g.forward(p * n_micro + f)

        @when(t < 2)
        def _():
            gather_h.forward(n_slots - 2 + t)

        @when(t == n_steps - 1, jnp.logical_not(is_first))
        def _():
            for slot in range(n_micro, n_micro + 2):
                load_slope(slot).start()

        @when(t == 0, is_last)
        def _():
            for k in range(1, n_stage):
                column_send(k).start()

        @when(t == 1)
        def _():
            @when(jnp.logical_not(is_last))
            def _():
                column_send(1).wait_recv()

            for k in range(len(place.plane)):
                plane_send(k).start()

        return carry

    lax.fori_loop(0, 2 * n_steps, bwd_step, 0)


    for k in range(len(place.plane)):
        plane_send(k).wait()
    total = parts[0]
    for k in range(1, n_data):
        total = total + parts[k]
    loss_ref[0, 0] = jnp.sum(total) / (2.0 * n_tok)

    @when(is_last)
    def _():
        for k in range(1, n_stage):
            column_send(k).wait_send()

    def drain_z(i, carry):
        bwd_whole(i + n_slots - 2 - n_micro * first).wait_send()
        return carry

    lax.fori_loop(0, 2, drain_z, 0)
    gather_h.drain(n_slots)
    gather_g.drain(n_slots)

    def drain_g(slot, carry):
        for k in range(4):
            gather_g.direct(slot, k).wait_send()
        return carry

    lax.fori_loop(0, n_slots, drain_g, 0)
    wait_sent(0)
    for v in range(2):
        for kind in range(2):
            for k, copy in enumerate(exchange(v, kind)):
                if k > 0:
                    copy().wait_recv()


def solution(mesh):
    n_stage = mesh.shape["stage"]
    n_data = mesh.shape["data"]

    def device_fn(tokens, targets, up, down):
        n_micro, seq_len, d_model = tokens.shape
        d_ff = up.shape[3]
        f_loc = d_ff // n_data
        n_slots = 2 * n_micro
        wide = -(-(d_model // 4 + (d_model // 4) % 128) // 128) * 128
        sizes = (d_model // 5, 2 * d_model // 5, 2 * d_model // 5) if d_model % 640 == 0 else (d_model // 2,) * 2
        pieces = tuple((sum(sizes[:k]), size) for k, size in enumerate(sizes))
        dma = pltpu.SemaphoreType.DMA
        hbm = pl.BlockSpec(memory_space=pl.ANY)
        vmem = pltpu.VMEM
        act_shape = (seq_len, d_model)
        gathered = jax.ShapeDtypeStruct((2, n_micro, n_data * seq_len, d_model), BF)
        spread = [dma((n_slots,)), dma((n_slots, 4)), dma((n_slots, 4)), dma((n_slots, 3)), dma((n_slots, 3))]
        grad_up, grad_down, loss, *_ = pl.pallas_call(
            functools.partial(kernel, n_stage, pieces),
            out_shape=(
                jax.ShapeDtypeStruct((2, 1, d_model // n_data, d_ff), F32),
                jax.ShapeDtypeStruct((2, 1, f_loc, d_model), F32),
                jax.ShapeDtypeStruct((1, 1), F32),
                gathered,
                gathered,
                jax.ShapeDtypeStruct((2, n_micro, seq_len, d_ff), F32),
            ),
            in_specs=[hbm] * 4,
            out_specs=(hbm, hbm, pl.BlockSpec(memory_space=pltpu.SMEM), hbm, hbm, hbm),
            scratch_shapes=[
                vmem((2, d_model, d_ff), BF),
                vmem((2, d_ff, d_model), BF),
                vmem((n_slots, *act_shape), BF),
                vmem((2, *act_shape), BF),
                vmem((seq_len, d_ff), BF),
                vmem((2, seq_len, d_ff), F32),
                vmem((seq_len, 128), F32),
                vmem((n_data, 8, 128), F32),
                vmem((f_loc, d_model), F32),
                vmem((d_model // 2, f_loc), F32),
                vmem((2, wide, f_loc), F32),
                dma((2, 4)), dma((2, 2)), dma((n_micro,)), dma, dma((2,)),
                dma((n_slots,)), dma((n_slots,)), dma((n_slots,)), dma((n_slots,)),
                dma((2, 2)), dma((2, 2)), dma((2,)), dma((2,)), dma, dma((2, 2)), dma((2, 6)), dma((2, 6)),
                dma((n_stage - 1,)), dma, dma((7,)), dma((7,)),
                *spread, *spread,
            ],
            compiler_params=pltpu.CompilerParams(collective_id=0, has_side_effects=True, vmem_limit_bytes=VMEM_BYTES),
            name="step",
        )(tokens, targets, up, down)
        return loss.reshape(()), grad_up, grad_down

    return jax.shard_map(
        device_fn,
        mesh=mesh,
        in_specs=(P("data"), P("data"), P(None, "stage"), P(None, "stage")),
        out_specs=(P(), P(None, "stage", "data"), P(None, "stage", "data")),
        check_vma=False,
    )
```
